768 devices in a mesh: section: 16 (over y, core), seq: 48 (over z, x).
Axes of the slice: x: 4, y: 8, z: 12, core: 2. Of those that a mesh axis runs over, the one named last changes fastest.
Arguments:
- stream: bfloat16 [16, 3072, 6144], P('section', 'seq'), may hold values from -1.5 to 1.5
- queries: bfloat16 [16, 3072, 6144], P('section', 'seq'), may hold values from -8 to 8
- key_rows: bfloat16 [16, 3072, 6144], P('section', 'seq'), may hold values from -8 to 8
- values: bfloat16 [16, 3072, 6144], P('section', 'seq'), may hold values from -36 to 36
- incoming: bfloat16 [3072, 6144], P('seq'), may hold values from -1.5 to 1.5
Outputs:
- updated: bfloat16 [16, 3072, 6144], P('section', 'seq')
- received: bfloat16 [16, 3072, 6144], P('section', 'seq')
The draws below stay inside these ranges and needn't reach their ends.
All inputs are finite; a program needn't handle non-finite values.
Results may differ from the reference program's by a relative error of at most 0.0054.
Values may be sent and summed in bfloat16 or wider, within the bound.
No kernel may reach another device: no remote copies, remote signals or barrier semaphores. Data moves between devices by JAX's collectives and lax.ppermute only.
A program may use at most 32 MiB of HBM per device.

```python
import jax
import jax.numpy as jnp
from jax import lax

HEAD_SIZE = 128
D = 6144
TOKENS = 3072
SEQ_LEN = 512
SEQS = 6
SECTIONS = 16


def make_pair(key):
    shape = (SECTIONS, TOKENS, D)
    query_key = jax.random.fold_in(key, 101)
    other_key = jax.random.fold_in(key, 102)
    queries = jnp.clip(jax.random.normal(query_key, shape, jnp.float32), -6.0, 6.0)
    keys_all = jnp.clip(jax.random.normal(other_key, shape, jnp.float32), -6.0, 6.0)
    return (queries, keys_all)


def draw_queries(key, part):
    return make_pair(key)[0].astype(jnp.bfloat16)


def draw_key_rows(key, part):
    return make_pair(key)[1].astype(jnp.bfloat16)


def steps_of(key, extent, shards, smallest, largest):
    gain, own = 1.0, jax.random.fold_in(key, 6)
    for dim, blocks in shards:
        steps = jnp.exp(jax.random.uniform(jax.random.fold_in(own, dim), (blocks,), jnp.float32, smallest / len(shards), largest / len(shards)))
        gain = gain * jnp.repeat(steps, extent[dim] // blocks).reshape([-1 if axis == dim else 1 for axis in range(len(extent))])
    return gain


def gaussian(rng, shape, deviation, limit, cuts=(), held_as=jnp.bfloat16):
    drawn = jax.random.normal(rng, shape, jnp.float32) * deviation
    if len(cuts) > 0:
        drawn = steps_of(rng, shape, cuts, -0.22, 0.18) * drawn
    return jnp.clip(drawn, min=-limit, max=limit).astype(held_as)


def setup_inputs(seed: int = 0) -> dict:
    key_of = jax.random.split(jax.random.key(seed), 6)
    return {
        "stream": gaussian(key_of[0], (SECTIONS, TOKENS, D), 0.25, 1.5, ((0, 16), (1, 48))),
        "queries": draw_queries(jax.random.fold_in(key_of[5], 71), 0),
        "key_rows": draw_key_rows(jax.random.fold_in(key_of[5], 71), 0),
        "values": gaussian(key_of[3], (SECTIONS, TOKENS, D), 6.0, 36.0, ((0, 16), (1, 48))),
        "incoming": gaussian(key_of[4], (TOKENS, D), 0.25, 1.5, ((0, 48),)),
    }


def attend_sequence(pieces):
    query_rows, key_rows, value_rows = pieces
    tok_count = query_rows.shape[0]
    head_count = query_rows.shape[1] // HEAD_SIZE
    query_f = query_rows.astype(jnp.float32).reshape(tok_count, head_count, HEAD_SIZE)
    key_f = key_rows.astype(jnp.float32).reshape(tok_count, head_count, HEAD_SIZE)
    value_f = value_rows.astype(jnp.float32).reshape(tok_count, head_count, HEAD_SIZE)
    scale = HEAD_SIZE ** -0.5
    scores = jnp.einsum("qhd,khd->hqk", query_f, key_f) * scale
    highest = jnp.max(scores, axis=-1, keepdims=True)
    exponent = jnp.exp(scores - highest)
    totals = jnp.sum(exponent, axis=-1)
    weights = lax.optimization_barrier(exponent.astype(jnp.bfloat16)).astype(jnp.float32)
    summed = jnp.einsum("hqk,khd->qhd", weights, value_f)
    attended = (summed / jnp.transpose(totals)[:, :, None]).astype(jnp.bfloat16)
    return attended.reshape(tok_count, head_count * HEAD_SIZE)


def attend_section(pieces):
    query_rows, key_rows, value_rows, stream_rows = pieces
    width = query_rows.shape[1]
    query_seq = query_rows.reshape(SEQS, SEQ_LEN, width)
    key_seq = key_rows.reshape(SEQS, SEQ_LEN, width)
    value_seq = value_rows.reshape(SEQS, SEQ_LEN, width)
    attended = lax.map(attend_sequence, (query_seq, key_seq, value_seq)).reshape(TOKENS, width)
    return (stream_rows.astype(jnp.float32) + attended.astype(jnp.float32)).astype(jnp.bfloat16)


def reference(stream, queries, key_rows, values, incoming):
    updated = lax.map(attend_section, (queries, key_rows, values, stream))
    received = jnp.concatenate([incoming[None], updated[:-1]], axis=0)
    return updated, received
```

```python
import math

import jax
import jax.numpy as jnp
from jax import lax
from jax.experimental import pallas as pl
from jax.experimental.pallas import tpu as pltpu
from jax.sharding import PartitionSpec as P

HEAD_SIZE = 128
GROUP = 8
DELAY = 8000
VMEM = pl.BlockSpec(memory_space=pltpu.VMEM)
SMEM = pl.BlockSpec(memory_space=pltpu.SMEM)
ANY = pl.BlockSpec(memory_space=pl.ANY)
SMALL = pltpu.CompilerParams(vmem_limit_bytes=16 << 20)


def pack_kernel(turns_ref, query_ref, key_ref, value_ref, out_ref, held, in_sems, out_sems):
    own = query_ref.shape[1] // GROUP
    incoming, outgoing = [], []
    for piece in range(GROUP):
        for part, ref in enumerate((query_ref, key_ref, value_ref)):
            incoming.append(
                pltpu.make_async_copy(
                    ref.at[:, pl.ds(piece * own, own)],
                    held.at[piece, :, pl.ds(part * own, own)],
                    in_sems.at[len(incoming)],
                )
            )
        outgoing.append(
            pltpu.make_async_copy(held.at[piece], out_ref.at[piece], out_sems.at[piece])
        )
    for copy in incoming:
        copy.start()
    for piece in range(GROUP):
        for copy in incoming[3 * piece : 3 * piece + 3]:
            copy.wait()
        outgoing[piece].start()
    for copy in outgoing:
        copy.wait()
    pl.delay(turns_ref[0])


def pack(turns, queries, key_rows, values):
    rows, width = queries.shape
    shape = (GROUP, rows, 3 * width // GROUP)
    return pl.pallas_call(
        pack_kernel,
        out_shape=jax.ShapeDtypeStruct(shape, queries.dtype),
        in_specs=[SMEM] + [ANY] * 3,
        out_specs=ANY,
        scratch_shapes=[
            pltpu.VMEM(shape, queries.dtype),
            pltpu.SemaphoreType.DMA((3 * GROUP,)),
            pltpu.SemaphoreType.DMA((GROUP,)),
        ],
        name="pack",
    )(turns, queries, key_rows, values)


def attend_kernel(in_ref, out_ref):
    pieces, rows, feats = out_ref.shape
    factor = HEAD_SIZE ** (-0.5) * math.log2(math.e)
    qkv = in_ref.reshape(pieces * rows, 3 * feats)
    for at in range(0, feats, HEAD_SIZE):
        query, key, value = (
            qkv[:, start : start + HEAD_SIZE] for start in (at, feats + at, 2 * feats + at)
        )
        scores = lax.dot_general(
            query, key, (((1,), (1,)), ((), ())), preferred_element_type=jnp.float32
        )
        highest = jnp.max(scores, axis=-1, keepdims=True)
        exponent = jnp.exp2((scores - highest) * factor)
        totals = jnp.sum(exponent, axis=-1, keepdims=True)
        summed = jnp.dot(exponent.astype(jnp.bfloat16), value, preferred_element_type=jnp.float32)
        attended = (summed / totals).astype(out_ref.dtype)
        out_ref[:, :, at : at + HEAD_SIZE] = attended.reshape(pieces, rows, HEAD_SIZE)


def attend(qkv):
    pieces, rows, width = qkv.shape
    return pl.pallas_call(
        attend_kernel,
        out_shape=jax.ShapeDtypeStruct((pieces, rows, width // 3), qkv.dtype),
        in_specs=[VMEM],
        out_specs=VMEM,
        compiler_params=SMALL,
        name="attend",
    )(qkv)


def update_kernel(last_ref, stream_ref, branch_ref, incoming_ref, updated_ref, sent_ref):
    own = branch_ref.shape[2]
    for piece in range(branch_ref.shape[0]):
        here = slice(piece * own, (piece + 1) * own)
        total = stream_ref[:, here].astype(jnp.float32) + branch_ref[piece].astype(jnp.float32)
        updated = total.astype(updated_ref.dtype)
        updated_ref[:, here] = updated
        sent_ref[:, here] = jnp.where(last_ref[0] == 1, incoming_ref[:, here], updated)


def update(stream, branch, incoming, is_last):
    return pl.pallas_call(
        update_kernel,
        out_shape=[jax.ShapeDtypeStruct(stream.shape, stream.dtype)] * 2,
        in_specs=[SMEM, VMEM, VMEM, VMEM],
        out_specs=[VMEM, VMEM],
        compiler_params=SMALL,
        name="update",
    )(is_last, stream, branch, incoming)


def pick_kernel(odd_ref, onto_odd_ref, onto_even_ref, out_ref, sem):
    @pl.when(odd_ref[0] == 1)
    def _():
        copy = pltpu.make_async_copy(onto_odd_ref, out_ref, sem)
        copy.start()
        copy.wait()

    @pl.when(odd_ref[0] == 0)
    def _():
        copy = pltpu.make_async_copy(onto_even_ref, out_ref, sem)
        copy.start()
        copy.wait()


def pick(is_odd, onto_odd, onto_even):
    return pl.pallas_call(
        pick_kernel,
        out_shape=jax.ShapeDtypeStruct(onto_odd.shape, onto_odd.dtype),
        in_specs=[SMEM, VMEM, VMEM],
        out_specs=ANY,
        scratch_shapes=[pltpu.SemaphoreType.DMA],
        compiler_params=SMALL,
        name="pick",
    )(is_odd, onto_odd, onto_even)


def exchange(pieces):
    count = lax.axis_size("seq")
    groups = [list(range(at, at + GROUP)) for at in range(0, count, GROUP)]
    return lax.all_to_all(
        pieces, "seq", split_axis=0, concat_axis=0, tiled=True, axis_index_groups=groups
    )


def per_device(stream, queries, key_rows, values, incoming):
    sections = lax.axis_size("section")
    section, index = lax.axis_index("section"), lax.axis_index("seq")
    is_last = (section == sections - 1).astype(jnp.int32)[None]
    waits = (section % 2 == 0) & (index % GROUP != 0)
    turns = jnp.where(waits, DELAY, 0).astype(jnp.int32)[None]
    gathered = exchange(pack(turns, queries[0], key_rows[0], values[0]))
    branch = exchange(attend(gathered))
    updated, sent = update(stream[0], branch, incoming, is_last)
    evens, odds = range(0, sections, 2), range(1, sections, 2)
    relayed = lax.ppermute(sent, "section", [(s, (s + 2) % sections) for s in odds])
    onto_odd = lax.ppermute(sent, "section", [(s, s + 1) for s in evens])
    onto_even = lax.ppermute(relayed, "section", [(s, s - 1) for s in odds])
    received = pick((section % 2)[None], onto_odd, onto_even)
    return (updated[None], received[None])


def solution(mesh):
    whole = P("section", "seq", None)
    return jax.shard_map(
        per_device,
        mesh=mesh,
        in_specs=(whole, whole, whole, whole, P("seq", None)),
        out_specs=(whole, whole),
        check_vma=False,
    )
```
